512 devices in a mesh: section: 4 (over z_hi), row: 4 (over z_lo, core), col: 32 (over y, x).
Axes of the slice: x: 4, y: 8, z: 8 (z_hi: 4, z_lo: 2; z = z_hi * 2 + z_lo), core: 2. Of those that a mesh axis runs over, the one named last changes fastest.
Arguments:
- state: bfloat16 [4, 128, 1024, 256], P('section', 'row', 'col'), may hold values from -6 to 6
- fresh: bfloat16 [128, 1024, 256], P('row', 'col'), may hold values from -6 to 6
- conv_first: bfloat16 [4, 3, 3, 256, 256], P('section'), may hold values from -0.125 to 0.125
- conv_second: bfloat16 [4, 3, 3, 256, 256], P('section'), may hold values from -0.125 to 0.125
- gains: float32 [4, 2, 256], P('section'), may hold values from 0.1 to 1.9
- shifts: float32 [4, 2, 256], P('section'), may hold values from -2.4 to 2.4
Outputs:
- blocks: bfloat16 [2, 4, 128, 1024, 256], P(None, 'section', 'row', 'col')
The draws below stay inside these ranges and needn't reach their ends.
All inputs are finite; a program needn't handle non-finite values.
Results may differ from the reference program's by a relative error of at most 0.005.
Values may be sent and summed in bfloat16 or wider, within the bound.
No kernel may reach another device: no remote copies, remote signals or barrier semaphores. Data moves between devices by JAX's collectives and lax.ppermute only.
A program may use at most 64 MiB of HBM per device.

```python
import jax
import jax.numpy as jnp
from jax import lax

C = 256
TICKS = 2
SECTIONS = 4
NH = 128
NW = 1024


def shard_levels(rng, extent, split, smallest, high):
    loudness, own = 1.0, jax.random.fold_in(rng, 6)
    for axis_at, parts in split:
        draws = jnp.exp(jax.random.uniform(jax.random.fold_in(own, axis_at), (parts,), jnp.float32, smallest / len(split), high / len(split)))
        loudness = loudness * jnp.repeat(draws, extent[axis_at] // parts).reshape([-1 if axis == axis_at else 1 for axis in range(len(extent))])
    return loudness


def gaussian(rng, dims, scale, reach, split=(), held_as=jnp.bfloat16):
    values = jax.random.normal(rng, dims, jnp.float32) * scale
    if len(split) > 0:
        values = shard_levels(rng, dims, split, -0.22, 0.18) * values
    return jnp.clip(values, min=-reach, max=reach).astype(held_as)


def setup_inputs(seed: int = 0) -> dict:
    key_of = jax.random.split(jax.random.key(seed), 7)
    return {
        "state": gaussian(key_of[0], (SECTIONS, NH, NW, C), 1.0, 6.0, ((0, 4), (1, 4), (2, 32))),
        "fresh": gaussian(key_of[1], (NH, NW, C), 1.0, 6.0, ((0, 4), (1, 32))),
        "conv_first": gaussian(key_of[2], (SECTIONS, 3, 3, C, C), (9 * C) ** -0.5, 0.125, ((0, 4),)),
        "conv_second": gaussian(key_of[3], (SECTIONS, 3, 3, C, C), (9 * C) ** -0.5, 0.125, ((0, 4),)),
        "gains": jnp.clip(1.0 + 0.18 * jax.random.normal(key_of[4], (SECTIONS, 2, C), jnp.float32), 0.1, 1.9),
        "shifts": gaussian(key_of[5], (SECTIONS, 2, C), 0.4, 2.4, ((0, 4),), jnp.float32),
    }


def convolve(features, kernel):
    result = lax.conv_general_dilated(features.astype(jnp.float32)[None], kernel.astype(jnp.float32), (1, 1), "SAME", dimension_numbers=("NHWC", "HWIO", "NHWC"), precision=lax.Precision.HIGHEST)
    return result[0]


def section_block(features, first_kernel, second_kernel, gain_pair, shift_pair):
    hidden = jax.nn.relu(gain_pair[0] * convolve(features, first_kernel) + shift_pair[0]).astype(jnp.bfloat16)
    summed = features.astype(jnp.float32) + gain_pair[1] * convolve(hidden, second_kernel) + shift_pair[1]
    return jax.nn.relu(summed).astype(jnp.bfloat16)


def reference(state, fresh, conv_first, conv_second, gains, shifts):
    current = [state[section_index] for section_index in range(SECTIONS)]
    per_tick = []
    for tick_index in range(TICKS):
        outputs = [section_block(current[section_index], conv_first[section_index], conv_second[section_index], gains[section_index], shifts[section_index]) for section_index in range(SECTIONS)]
        per_tick.append(jnp.stack(outputs))
        current = [fresh] + outputs[:-1]
    return jnp.stack(per_tick)
```

```python
import functools

import jax
import jax.numpy as jnp
from jax import lax
from jax.experimental import pallas as pl
from jax.experimental.pallas import tpu as pltpu
from jax.sharding import PartitionSpec as P

TICKS = 2
BF16 = jnp.bfloat16
F32 = jnp.float32
BLOCK = 8


def edge_rows(x, axis_name):
    count = lax.axis_size(axis_name)
    forward = [(i, i + 1) for i in range(count - 1)]
    backward = [(target, source) for source, target in forward]
    low = lax.ppermute(x[-2:], axis_name, forward)
    high = lax.ppermute(x[:2], axis_name, backward)
    return low, high


def edge_cols(x, low, high, axis_name):
    count = lax.axis_size(axis_name)
    forward = [(i, i + 1) for i in range(count - 1)]
    backward = [(target, source) for source, target in forward]
    tall_right = jnp.concatenate([low[:, -2:], x[:, -2:], high[:, -2:]], axis=0)
    tall_left = jnp.concatenate([low[:, :2], x[:, :2], high[:, :2]], axis=0)
    left = lax.ppermute(tall_right, axis_name, forward)
    right = lax.ppermute(tall_left, axis_name, backward)
    return left, right


def shifted(x, axis, by):
    devices = lax.axis_size(axis)
    pairs = [(i, i + by) for i in range(devices) if 0 <= i + by < devices]
    return lax.ppermute(x, axis, pairs)


def tick_kernel(
    flags, x, top, bot, left, right, k1, k2, gains, shifts, out, x3, h3, edge, hedge, *, first, count
):
    rows, cols, chan = x.shape
    half = hedge.shape[0] // 2
    iota = lax.broadcasted_iota(jnp.int32, (cols, 1), 0)

    def stack(source, index, p):
        at = p - first
        wide = source[index]
        row = wide.astype(F32)
        lo = left[p].astype(F32)
        hi = right[p].astype(F32)
        spot = pl.multiple_of(at * cols, cols)
        x3[pl.ds(spot, cols), 0:chan] = jnp.where(iota == 0, lo[1:2], pltpu.roll(row, 1, 0)).astype(BF16)
        x3[pl.ds(spot, cols), chan : 2 * chan] = wide
        x3[pl.ds(spot, cols), 2 * chan :] = jnp.where(
            iota == cols - 1, hi[0:1], pltpu.roll(row, cols - 1, 0)
        ).astype(BF16)
        edge[pl.ds(at, 1), 0:chan] = lo[0:1]
        edge[pl.ds(at, 1), chan : 2 * chan] = lo[1:2]
        edge[pl.ds(at, 1), 2 * chan :] = row[0:1]
        edge[pl.ds(half + at, 1), 0:chan] = row[cols - 1 : cols]
        edge[pl.ds(half + at, 1), chan : 2 * chan] = hi[0:1]
        edge[pl.ds(half + at, 1), 2 * chan :] = hi[1:2]

    edge[...] = jnp.zeros(edge.shape, F32)
    for p in range(first, min(2, first + count + 4)):
        stack(top, p, p)
    start = max(first, 2)
    stop = min(first + count + 4, rows + 2)

    @pl.loop(start, stop)
    def _(p):
        stack(x, p - 2, p)

    for p in range(max(first, rows + 2), first + count + 4):
        stack(bot, p - rows - 2, p)

    gain1, shift1 = gains[0:1], shifts[0:1]
    gain2, shift2 = gains[1:2], shifts[1:2]
    wide_edge = edge[...].astype(BF16)
    total = None
    for tap in range(3):
        part = jnp.dot(wide_edge, k1[pl.ds(tap * 3 * chan, 3 * chan)], preferred_element_type=F32)
        if tap:
            part = pltpu.roll(part, 2 * half - tap, 0)
        total = part if total is None else total + part
    spots = lax.broadcasted_iota(jnp.int32, (2 * half, 1), 0)
    side = spots >= half
    hid_row = first - 1 + jnp.where(side, spots - half, spots)
    keep_row = ((hid_row >= 0) | (flags[0] == 0)) & ((hid_row < rows) | (flags[1] == 0))
    keep_col = (side & (flags[3] == 0)) | (jnp.logical_not(side) & (flags[2] == 0))
    hedge[...] = jnp.where(keep_row & keep_col, jnp.maximum(gain1 * total + shift1, 0.0), 0.0)

    def hidden_block(i, size):
        spot = pl.multiple_of(i * cols, cols)
        acc = None
        for tap in range(3):
            part = jnp.dot(
                x3[pl.ds(spot + tap * cols, size * cols), :],
                k1[pl.ds(tap * 3 * chan, 3 * chan)],
                preferred_element_type=F32,
            )
            acc = part if acc is None else acc + part
        acc = jnp.maximum(gain1 * acc + shift1, 0.0)
        for r in range(size):
            row_id = first - 1 + i + r
            keep = ((row_id >= 0) | (flags[0] == 0)) & ((row_id < rows) | (flags[1] == 0))
            row = jnp.where(keep, acc[r * cols : (r + 1) * cols], 0.0)
            lo = hedge[pl.ds(i + r, 1)]
            hi = hedge[pl.ds(half + i + r, 1)]
            here = pl.ds(spot + r * cols, cols)
            h3[here, 0:chan] = jnp.where(iota == 0, lo, pltpu.roll(row, 1, 0)).astype(BF16)
            h3[here, chan : 2 * chan] = row.astype(BF16)
            h3[here, 2 * chan :] = jnp.where(iota == cols - 1, hi, pltpu.roll(row, cols - 1, 0)).astype(BF16)

    def output_block(i, size):
        spot = pl.multiple_of(i * cols, cols)
        acc = None
        for tap in range(3):
            part = jnp.dot(
                h3[pl.ds(spot + tap * cols, size * cols), :],
                k2[pl.ds(tap * 3 * chan, 3 * chan)],
                preferred_element_type=F32,
            )
            acc = part if acc is None else acc + part
        acc = (gain2 * acc + shift2).reshape(size, cols, chan)
        base = x[pl.ds(first + i, size)].astype(F32)
        out[pl.ds(i, size)] = jnp.maximum(base + acc, 0.0).astype(BF16)

    def blocks(total_rows, body):
        whole = total_rows // BLOCK

        @pl.loop(0, whole)
        def _(b):
            body(b * BLOCK, BLOCK)

        if total_rows % BLOCK:
            body(whole * BLOCK, total_rows % BLOCK)

    blocks(count + 2, hidden_block)
    blocks(count, output_block)


def tick_call(flags, x, low, high, left, right, k1, k2, gains, shifts, first, count):
    rows, cols, chan = x.shape
    half = -(-(count + 4) // 8) * 8
    vmem = pl.BlockSpec(memory_space=pltpu.VMEM)
    return pl.pallas_call(
        functools.partial(tick_kernel, first=first, count=count),
        out_shape=jax.ShapeDtypeStruct((count, cols, chan), BF16),
        in_specs=[pl.BlockSpec(memory_space=pltpu.SMEM)] + [vmem] * 9,
        out_specs=vmem,
        scratch_shapes=[
            pltpu.VMEM(((count + 4) * cols, 3 * chan), BF16),
            pltpu.VMEM(((count + 2) * cols, 3 * chan), BF16),
            pltpu.VMEM((2 * half, 3 * chan), F32),
            pltpu.VMEM((2 * half, chan), F32),
        ],
        compiler_params=pltpu.CompilerParams(vmem_limit_bytes=24 * 1024 * 1024),
        name=f"tick_{first}_{count}",
    )(flags, x, low, high, left, right, k1, k2, gains, shifts)


def per_device(state, fresh, conv_first, conv_second, gains, shifts):
    chan = state.shape[-1]
    k1 = conv_first[0].reshape(9 * chan, chan)
    k2 = conv_second[0].reshape(9 * chan, chan)
    row, col = lax.axis_index("row"), lax.axis_index("col")
    flags = jnp.stack(
        [row == 0, row == lax.axis_size("row") - 1, col == 0, col == lax.axis_size("col") - 1]
    ).astype(jnp.int32)
    features = state[0]
    results = []
    for tick_index in range(TICKS):
        low, high = edge_rows(features, "row")
        left, right = edge_cols(features, low, high, "col")
        output = tick_call(
            flags, features, low, high, left, right, k1, k2, gains[0], shifts[0], 0, features.shape[0]
        )
        results.append(output)
        if tick_index + 1 < TICKS:
            arrived = shifted(output, "section", 1)
            features = jnp.where(lax.axis_index("section") == 0, fresh, arrived)
    return jnp.stack(results)[:, None]


def solution(mesh):
    in_specs = (
        P("section", "row", "col", None),
        P("row", "col", None),
        P("section", None, None, None, None),
        P("section", None, None, None, None),
        P("section", None, None),
        P("section", None, None),
    )
    out_specs = P(None, "section", "row", "col", None)
    return jax.shard_map(
        per_device, mesh=mesh, in_specs=in_specs, out_specs=out_specs, check_vma=False
    )
```

```python
import functools

import jax
import jax.numpy as jnp
from jax import lax
from jax.experimental import pallas as pl
from jax.experimental.pallas import tpu as pltpu
from jax.sharding import PartitionSpec as P


BF16 = jnp.bfloat16
F32 = jnp.float32
VMEM_LIMIT = 24 * 1024 * 1024
SIDE = 16
MOST = 19


def largest_divisor(n, most):
    return next(d for d in range(most, 0, -1) if n % d == 0)


def dots(source, spot, size, pitch, weights):
    chan = weights.shape[1]
    acc = None
    for tap in range(3):
        part = jnp.dot(
            source[pl.ds(pl.multiple_of(spot + tap * pitch, 8), size * pitch), :],
            weights[pl.ds(tap * 3 * chan, 3 * chan), :],
            preferred_element_type=F32,
        )
        acc = part if acc is None else acc + part
    return acc


def stack_row(x3, at, row):
    pitch, chan = row.shape
    spot = pl.ds(pl.multiple_of(at * pitch, 8), pitch)
    x3[spot, 0:chan] = pltpu.roll(row, 1, 0).astype(BF16)
    x3[spot, chan : 2 * chan] = row.astype(BF16)
    x3[spot, 2 * chan :] = pltpu.roll(row, pitch - 1, 0).astype(BF16)


def kept(flags, extent, row_id, col_keep):
    inside = ((row_id >= 0) | (flags[0] == 0)) & ((row_id < extent) | (flags[1] == 0))
    return col_keep & inside


def wide_keep(flags, pitch, reach):
    j = lax.broadcasted_iota(jnp.int32, (pitch, 1), 0)
    low, high = j < reach, j >= pitch - reach
    return jnp.logical_not(low & (flags[2] == 1)) & jnp.logical_not(high & (flags[3] == 1))


def convolutions(flags, extent, pitch, reach, first, count, x3, h3, weights, emit):
    gains, shifts, k1, k2 = weights
    chan = k1.shape[1]
    col_keep = wide_keep(flags, pitch, reach)
    gain1, shift1 = gains[0:1], shifts[0:1]
    gain2, shift2 = gains[1:2], shifts[1:2]
    size1 = largest_divisor(count + 2, MOST)

    def hidden_block(b):
        spot = b * (size1 * pitch)
        acc = jnp.maximum(gain1 * dots(x3, spot, size1, pitch, k1) + shift1, 0.0)
        for r in range(size1):
            keep = kept(flags, extent, first - 1 + b * size1 + r, col_keep)
            stack_row(h3, b * size1 + r, jnp.where(keep, acc[r * pitch : (r + 1) * pitch], 0.0))

    pl.loop(0, (count + 2) // size1)(hidden_block)
    size2 = largest_divisor(count, MOST)
    for b in range(count // size2):
        i = b * size2
        acc = gain2 * dots(h3, i * pitch, size2, pitch, k2) + shift2
        base = x3[pl.ds((i + 2) * pitch, size2 * pitch), chan : 2 * chan].astype(F32)
        acc = jnp.maximum(base + acc, 0.0)
        values = []
        for r in range(size2):
            keep = kept(flags, extent, first + i + r, col_keep)
            values.append(jnp.where(keep, acc[r * pitch : (r + 1) * pitch], 0.0))
        emit(i, values)


def run_copies(pairs, sems):
    copies = [pltpu.make_async_copy(a, b, sems.at[n]) for n, (a, b) in enumerate(pairs)]
    for copy in copies:
        copy.start()
    for copy in copies:
        copy.wait()


def edge_kernel(x, fresh, down, up, sems):
    rows = x.shape[0]
    run_copies(
        (
            (x.at[pl.ds(rows - 4, 4)], down.at[pl.ds(0, 4)]),
            (fresh.at[pl.ds(rows - 2, 2)], down.at[pl.ds(4, 2)]),
            (x.at[pl.ds(0, 4)], up.at[pl.ds(0, 4)]),
            (fresh.at[pl.ds(0, 2)], up.at[pl.ds(4, 2)]),
        ),
        sems,
    )


def load_kernel(*refs):
    half = (len(refs) - 1) // 2
    fresh, sources, targets = refs[0], refs[1:half], refs[half:-1]
    cols = fresh.shape[1]
    sides = ((fresh.at[:, pl.ds(at, 8)], targets[n]) for n, at in enumerate((0, cols - 8)))
    run_copies((*sides, *zip(sources, targets[2:])), refs[-1])


def pack_kernel(x, fresh_low, fresh_high, top, bot, to_right, to_left, packed):
    rows, cols, _ = x.shape
    wide = 4 * (rows + 8)
    for side, out in ((1, to_right), (0, to_left)):
        edge = pl.ds((cols - 8) * side, 8)
        for n, (halo, keep) in enumerate(((4, 4), (2, 2))):
            for p in range(rows + 2 * halo):
                at = p - halo
                if at < 0:
                    piece = top[4 * n + p, edge]
                elif at >= rows:
                    piece = bot[4 * n + at - rows, edge]
                else:
                    piece = (fresh_low, fresh_high)[side][at] if n else x[at, edge]
                piece = piece.astype(F32)
                piece = piece[8 - keep :] if side else piece[:keep]
                spot = wide * n + keep * p
                packed[spot : spot + keep] = piece
        out[...] = packed[...].astype(BF16)


def extended_row(x, top, bot, at, halo, skip):
    rows = x.shape[0]
    if at < 0:
        return top[skip + halo + at].astype(F32)
    if at >= rows:
        return bot[skip + at - rows].astype(F32)
    return x[at].astype(F32)


def main_kernel(flags, x, top, bot, gains, shifts, k1, k2, msg, x3, h3, inner):
    rows, cols, _ = x.shape
    keep = cols - 4
    for p in range(rows + 8):
        stack_row(x3, p, extended_row(x, top, bot, p - 4, 4, 0))

    def emit(i, values):
        for r, value in enumerate(values):
            inner[(i + r) * keep : (i + r + 1) * keep] = value[2 : cols - 2]

    weights = gains, shifts, k1, k2
    convolutions(flags, rows, cols, 0, -2, rows + 4, x3, h3, weights, emit)
    msg[...] = inner[...].astype(BF16)


def side_kernel(flags, x, top, bot, left, right, gains, shifts, k1, k2, msg, x3, h3, es, row):
    rows, cols, _ = x.shape
    for p in range(rows + 8):
        main = extended_row(x, top, bot, p - 4, 4, 0)
        row[p, 0:4] = left[4 * p : 4 * p + 4].astype(F32)
        row[p, 4:8] = main[0:4]
        row[p, 8:12] = main[cols - 4 : cols]
        row[p, 12:16] = right[4 * p : 4 * p + 4].astype(F32)
        stack_row(x3, p, row[p])

    def emit(i, values):
        for r, value in enumerate(values):
            n = i + r
            es[8 * n : 8 * n + 4] = value[2:6]
            es[8 * n + 4 : 8 * n + 8] = value[10:14]

    weights = gains, shifts, k1, k2
    convolutions(flags, rows, SIDE, 4, -2, rows + 4, x3, h3, weights, emit)
    msg[...] = es[...].astype(BF16)


def keep_kernel(main, sides, blocks, osc, row, sem, *, rows, cols):
    inner = cols - 4
    for n in range(rows):
        p = n + 2
        edge = sides[8 * p : 8 * p + 8].astype(F32)
        row[n, 0:2] = edge[2:4]
        row[n, 2 : cols - 2] = main[inner * p : inner * (p + 1)].astype(F32)
        row[n, cols - 2 : cols] = edge[4:6]
        osc[n * cols : (n + 1) * cols] = row[n].astype(BF16)
    copy = pltpu.make_async_copy(osc, blocks.at[pl.ds(0, rows * cols)], sem)
    copy.start()
    copy.wait()


def late_main_kernel(flags, main, fresh, top, bot, gains, shifts, k1, k2, out, x3, h3, row):
    rows, cols, chan = fresh.shape
    inner = cols - 4

    @pl.when(flags[4] == 1)
    def _():
        for p in range(rows + 4):
            row[p] = extended_row(fresh, top, bot, p - 2, 2, 4)

    @pl.when(flags[4] == 0)
    def _():
        for p in range(rows + 4):
            row[p, 0:2] = jnp.zeros((2, chan), F32)
            row[p, 2 : cols - 2] = main[inner * p : inner * (p + 1)].astype(F32)
            row[p, cols - 2 : cols] = jnp.zeros((2, chan), F32)

    for p in range(rows + 4):
        stack_row(x3, p, row[p])

    def emit(i, values):
        for r, value in enumerate(values):
            out[(i + r) * cols : (i + r + 1) * cols] = value.astype(BF16)

    weights = gains, shifts, k1, k2
    convolutions(flags, rows, cols, 0, 0, rows, x3, h3, weights, emit)


def late_side_kernel(
    flags, main, sides, middle, fresh, top, bot, left, right, gains, shifts, k1, k2, _, blocks, x3, h3, row,
    full, osc, sems
):
    rows, cols, _ = fresh.shape
    inner = cols - 4
    wide = 4 * (rows + 8)

    @pl.when(flags[4] == 1)
    def _():
        for p in range(rows + 4):
            own = extended_row(fresh, top, bot, p - 2, 2, 4)
            spot = wide + 2 * p
            row[p, 0:2] = left[spot : spot + 2].astype(F32)
            row[p, 2:8] = own[0:6]
            row[p, 8:14] = own[cols - 6 : cols]
            row[p, 14:16] = right[spot : spot + 2].astype(F32)

    @pl.when(flags[4] == 0)
    def _():
        for p in range(rows + 4):
            edge = sides[8 * p : 8 * p + 8].astype(F32)
            row[p, 0:4] = edge[0:4]
            row[p, 4:8] = main[inner * p : inner * p + 4].astype(F32)
            row[p, 8:12] = main[inner * (p + 1) - 4 : inner * (p + 1)].astype(F32)
            row[p, 12:16] = edge[4:8]

    for p in range(rows + 4):
        stack_row(x3, p, row[p])
    copies = []

    def emit(i, values):
        for r, value in enumerate(values):
            n = i + r
            here = slice(n * cols, (n + 1) * cols)
            full[n] = middle[here].astype(F32)
            full[n, 0:4] = value[2:6]
            full[n, cols - 4 : cols] = value[10:14]
            osc[here] = full[n].astype(BF16)
        size = len(values) * cols
        copy = pltpu.make_async_copy(
            osc.at[pl.ds(i * cols, size)],
            blocks.at[pl.ds((rows + i) * cols, size)],
            sems.at[len(copies)],
        )
        copy.start()
        copies.append(copy)

    weights = gains, shifts, k1, k2
    convolutions(flags, rows, SIDE, 2, 0, rows, x3, h3, weights, emit)
    for copy in copies:
        copy.wait()


SMEM = pl.BlockSpec(memory_space=pltpu.SMEM)
VM = pl.BlockSpec(memory_space=pltpu.VMEM)
ANY = pl.BlockSpec(memory_space=pl.ANY)
HBM = pl.BlockSpec(memory_space=pltpu.HBM)
PARAMS = dict(vmem_limit_bytes=VMEM_LIMIT)


def cost(count, pitch, chan):
    return pl.CostEstimate(
        flops=4 * 9 * count * pitch * chan * chan, bytes_accessed=3 * 1024 * 1024, transcendentals=0
    )


def tick_call(body, operands, out_shape, count, pitch, scratch, last=False):
    chan = out_shape[1]
    stacks = [
        pltpu.VMEM(((count + 4) * pitch, 3 * chan), BF16),
        pltpu.VMEM(((count + 2) * pitch, 3 * chan), BF16),
    ]
    spaces = [SMEM] + [VM] * (len(operands) - 1)
    if last:
        spaces[-1] = HBM
    return pl.pallas_call(
        body,
        out_shape=jax.ShapeDtypeStruct(out_shape, BF16),
        in_specs=spaces,
        out_specs=HBM if last else VM,
        scratch_shapes=stacks + scratch,
        input_output_aliases={len(operands) - 1: 0} if last else {},
        compiler_params=pltpu.CompilerParams(**PARAMS),
        cost_estimate=cost(count, pitch, chan),
    )(*operands)


def edge_call(x, fresh):
    shape = jax.ShapeDtypeStruct((6,) + x.shape[1:], BF16)
    return pl.pallas_call(
        edge_kernel,
        out_shape=[shape, shape],
        in_specs=[HBM, HBM],
        out_specs=[VM, VM],
        scratch_shapes=[pltpu.SemaphoreType.DMA((4,))],
        compiler_params=pltpu.CompilerParams(**PARAMS),
        name="edge",
    )(x, fresh)


def load_call(fresh, values):
    rows, _, chan = fresh.shape
    shapes = [(rows, 8, chan)] * 2 + [v.shape for v in values]
    kinds = [BF16] * 2 + [v.dtype for v in values]
    return pl.pallas_call(
        load_kernel,
        out_shape=[jax.ShapeDtypeStruct(shape, kind) for shape, kind in zip(shapes, kinds)],
        in_specs=[HBM] * (len(values) + 1),
        out_specs=[VM] * len(shapes),
        scratch_shapes=[pltpu.SemaphoreType.DMA((len(shapes),))],
        compiler_params=pltpu.CompilerParams(**PARAMS),
        cost_estimate=pl.CostEstimate(flops=1 << 30, bytes_accessed=4 << 20, transcendentals=0),
        name="load",
    )(fresh, *values)


def pack_call(x, sides, top, bot):
    rows, _, chan = x.shape
    total = 4 * (rows + 8) + 2 * (rows + 4)
    return pl.pallas_call(
        pack_kernel,
        out_shape=[jax.ShapeDtypeStruct((total, chan), BF16)] * 2,
        in_specs=[VM] * 5,
        out_specs=[VM, VM],
        scratch_shapes=[pltpu.VMEM((total, chan), F32)],
        compiler_params=pltpu.CompilerParams(**PARAMS),
        name="pack",
    )(x, *sides, top, bot)


def keep_call(main, sides, shape):
    rows, cols, chan = shape
    return pl.pallas_call(
        functools.partial(keep_kernel, rows=rows, cols=cols),
        out_shape=jax.ShapeDtypeStruct((2 * rows * cols, chan), BF16),
        in_specs=[VM, VM],
        out_specs=HBM,
        scratch_shapes=[
            pltpu.VMEM((rows * cols, chan), BF16),
            pltpu.VMEM((rows, cols, chan), F32),
            pltpu.SemaphoreType.DMA,
        ],
        compiler_params=pltpu.CompilerParams(**PARAMS),
        name="keep",
    )(main, sides)


def moves(axis, by):
    size = lax.axis_size(axis)
    return [(i, i + by) for i in range(size) if 0 <= i + by < size]


def tied(value, after):
    return lax.optimization_barrier((value, after))[0]


def in_hbm(value):
    return pltpu.with_memory_space_constraint(value, pltpu.HBM)


def per_device(state, fresh, conv_first, conv_second, gains, shifts):
    x = state[0]
    rows, cols, chan = x.shape
    flat = (9 * chan, chan)
    values = (fresh, x, gains[0], shifts[0], conv_first[0].reshape(flat), conv_second[0].reshape(flat))
    values = [in_hbm(v) for v in values]
    row, col = lax.axis_index("row"), lax.axis_index("col")
    flags = jnp.stack(
        [
            row == 0,
            row == lax.axis_size("row") - 1,
            col == 0,
            col == lax.axis_size("col") - 1,
            lax.axis_index("section") == 0,
        ]
    ).astype(jnp.int32)
    down, up = edge_call(values[1], values[0])
    bot = lax.ppermute(up, "row", moves("row", -1))
    top = lax.ppermute(down, "row", moves("row", 1))
    *sides, x, gain, shift, k1, k2 = load_call(values[0], values[1:])
    params = gain, shift, k1, k2
    tall = rows + 4

    def rows_of(*shape):
        return pltpu.VMEM((*shape, chan), F32)

    inner = tall * (cols - 4)
    operands = (flags, x, top, bot, *params)
    main = tick_call(main_kernel, operands, (inner, chan), tall, cols, [rows_of(inner)])

    def onward(message):
        return lax.ppermute(message, "section", moves("section", 1))

    got_main = onward(main)
    to_right, to_left = pack_call(x, sides, tied(top, main), bot)
    left = lax.ppermute(to_right, "col", moves("col", 1))
    right = lax.ppermute(to_left, "col", moves("col", -1))
    operands = (flags, x, top, bot, left, right, *params)
    scratch = [rows_of(8 * tall), rows_of(rows + 8, SIDE)]
    side = tick_call(side_kernel, operands, (8 * tall, chan), tall, SIDE, scratch)
    got_side = onward(side)
    blocks = keep_call(main, side, x.shape)
    operands = (flags, got_main, fresh, top, bot, *params)
    scratch = [rows_of(tall, cols)]
    shape = (rows * cols, chan)
    middle = tick_call(late_main_kernel, operands, shape, rows, cols, scratch)
    operands = (flags, got_main, got_side, middle, fresh, top, bot, left, right, *params, blocks)
    scratch = [
        rows_of(tall, SIDE),
        rows_of(rows, cols),
        pltpu.VMEM((rows * cols, chan), BF16),
        pltpu.SemaphoreType.DMA((rows,)),
    ]
    blocks = tick_call(late_side_kernel, operands, blocks.shape, rows, SIDE, scratch, last=True)
    return blocks.reshape(2, 1, rows, cols, chan)


def solution(mesh):
    in_specs = (
        P("section", "row", "col", None),
        P("row", "col", None),
        P("section", None, None, None, None),
        P("section", None, None, None, None),
        P("section", None, None),
        P("section", None, None),
    )
    out_specs = P(None, "section", "row", "col", None)
    return jax.shard_map(
        per_device, mesh=mesh, in_specs=in_specs, out_specs=out_specs, check_vma=False
    )
```

```python
import functools

import jax
import jax.numpy as jnp
from jax import lax
from jax.experimental import pallas as pl
from jax.experimental.pallas import tpu as pltpu
from jax.sharding import PartitionSpec as P


BF16 = jnp.bfloat16
F32 = jnp.float32
VMEM_LIMIT = 24 * 1024 * 1024
SIDE = 16
MOST = 19


def largest_divisor(n, most):
    return next(d for d in range(most, 0, -1) if n % d == 0)


def dots(source, spot, size, pitch, weights):
    chan = weights.shape[1]
    acc = None
    for tap in range(3):
        part = jnp.dot(
            source[pl.ds(pl.multiple_of(spot + tap * pitch, 8), size * pitch), :],
            weights[pl.ds(tap * 3 * chan, 3 * chan), :],
            preferred_element_type=F32,
        )
        acc = part if acc is None else acc + part
    return acc


def stack_row(x3, at, row):
    pitch, chan = row.shape
    spot = pl.ds(pl.multiple_of(at * pitch, 8), pitch)
    x3[spot, 0:chan] = pltpu.roll(row, 1, 0).astype(BF16)
    x3[spot, chan : 2 * chan] = row.astype(BF16)
    x3[spot, 2 * chan :] = pltpu.roll(row, pitch - 1, 0).astype(BF16)


def kept(flags, extent, row_id, col_keep):
    inside = ((row_id >= 0) | (flags[0] == 0)) & ((row_id < extent) | (flags[1] == 0))
    return col_keep & inside


def wide_keep(flags, pitch, reach):
    j = lax.broadcasted_iota(jnp.int32, (pitch, 1), 0)
    low, high = j < reach, j >= pitch - reach
    return jnp.logical_not(low & (flags[2] == 1)) & jnp.logical_not(high & (flags[3] == 1))


def convolutions(flags, extent, pitch, reach, first, count, x3, h3, weights, emit):
    gains, shifts, k1, k2 = weights
    chan = k1.shape[1]
    col_keep = wide_keep(flags, pitch, reach)
    gain1, shift1 = gains[0:1], shifts[0:1]
    gain2, shift2 = gains[1:2], shifts[1:2]
    size1 = largest_divisor(count + 2, MOST)

    def hidden_block(b):
        spot = b * (size1 * pitch)
        acc = jnp.maximum(gain1 * dots(x3, spot, size1, pitch, k1) + shift1, 0.0)
        for r in range(size1):
            keep = kept(flags, extent, first - 1 + b * size1 + r, col_keep)
            stack_row(h3, b * size1 + r, jnp.where(keep, acc[r * pitch : (r + 1) * pitch], 0.0))

    pl.loop(0, (count + 2) // size1)(hidden_block)
    size2 = largest_divisor(count, MOST)
    for b in range(count // size2):
        i = b * size2
        acc = gain2 * dots(h3, i * pitch, size2, pitch, k2) + shift2
        base = x3[pl.ds((i + 2) * pitch, size2 * pitch), chan : 2 * chan].astype(F32)
        acc = jnp.maximum(base + acc, 0.0)
        values = []
        for r in range(size2):
            keep = kept(flags, extent, first + i + r, col_keep)
            values.append(jnp.where(keep, acc[r * pitch : (r + 1) * pitch], 0.0))
        emit(i, values)


def run_copies(pairs, sems):
    copies = [pltpu.make_async_copy(a, b, sems.at[n]) for n, (a, b) in enumerate(pairs)]
    for copy in copies:
        copy.start()
    for copy in copies:
        copy.wait()


def edge_kernel(x, fresh, down, up, sems):
    rows = x.shape[0]
    run_copies(
        (
            (x.at[pl.ds(rows - 4, 4)], down.at[pl.ds(0, 4)]),
            (fresh.at[pl.ds(rows - 2, 2)], down.at[pl.ds(4, 2)]),
            (x.at[pl.ds(0, 4)], up.at[pl.ds(0, 4)]),
            (fresh.at[pl.ds(0, 2)], up.at[pl.ds(4, 2)]),
        ),
        sems,
    )


def load_kernel(*refs):
    half = (len(refs) - 1) // 2
    fresh, sources, targets = refs[0], refs[1:half], refs[half:-1]
    cols = fresh.shape[1]
    sides = ((fresh.at[:, pl.ds(at, 8)], targets[n]) for n, at in enumerate((0, cols - 8)))
    run_copies((*sides, *zip(sources, targets[2:])), refs[-1])


def pack_kernel(x, fresh_low, fresh_high, top, bot, to_right, to_left, packed):
    rows, cols, _ = x.shape
    wide = 4 * (rows + 8)
    for side, out in ((1, to_right), (0, to_left)):
        edge = pl.ds((cols - 8) * side, 8)
        for n, (halo, keep) in enumerate(((4, 4), (2, 2))):
            for p in range(rows + 2 * halo):
                at = p - halo
                if at < 0:
                    piece = top[4 * n + p, edge]
                elif at >= rows:
                    piece = bot[4 * n + at - rows, edge]
                else:
                    piece = (fresh_low, fresh_high)[side][at] if n else x[at, edge]
                piece = piece.astype(F32)
                piece = piece[8 - keep :] if side else piece[:keep]
                spot = wide * n + keep * p
                packed[spot : spot + keep] = piece
        out[...] = packed[...].astype(BF16)


def extended_row(x, top, bot, at, halo, skip):
    rows = x.shape[0]
    if at < 0:
        return top[skip + halo + at].astype(F32)
    if at >= rows:
        return bot[skip + at - rows].astype(F32)
    return x[at].astype(F32)


def main_kernel(flags, x, top, bot, gains, shifts, k1, k2, msg, x3, h3, inner):
    rows, cols, _ = x.shape
    keep = cols - 4
    for p in range(rows + 8):
        stack_row(x3, p, extended_row(x, top, bot, p - 4, 4, 0))

    def emit(i, values):
        for r, value in enumerate(values):
            inner[(i + r) * keep : (i + r + 1) * keep] = value[2 : cols - 2]

    weights = gains, shifts, k1, k2
    convolutions(flags, rows, cols, 0, -2, rows + 4, x3, h3, weights, emit)
    msg[...] = inner[...].astype(BF16)


def side_kernel(flags, x, top, bot, left, right, gains, shifts, k1, k2, msg, x3, h3, es, row):
    rows, cols, _ = x.shape
    for p in range(rows + 8):
        main = extended_row(x, top, bot, p - 4, 4, 0)
        row[p, 0:4] = left[4 * p : 4 * p + 4].astype(F32)
        row[p, 4:8] = main[0:4]
        row[p, 8:12] = main[cols - 4 : cols]
        row[p, 12:16] = right[4 * p : 4 * p + 4].astype(F32)
        stack_row(x3, p, row[p])

    def emit(i, values):
        for r, value in enumerate(values):
            n = i + r
            es[8 * n : 8 * n + 4] = value[2:6]
            es[8 * n + 4 : 8 * n + 8] = value[10:14]

    weights = gains, shifts, k1, k2
    convolutions(flags, rows, SIDE, 4, -2, rows + 4, x3, h3, weights, emit)
    msg[...] = es[...].astype(BF16)


def keep_kernel(main, sides, blocks, osc, row, sem, *, rows, cols):
    inner = cols - 4
    for n in range(rows):
        p = n + 2
        edge = sides[8 * p : 8 * p + 8].astype(F32)
        row[n, 0:2] = edge[2:4]
        row[n, 2 : cols - 2] = main[inner * p : inner * (p + 1)].astype(F32)
        row[n, cols - 2 : cols] = edge[4:6]
        osc[n] = row[n].astype(BF16)
    copy = pltpu.make_async_copy(osc, blocks.at[pl.ds(0, rows)], sem)
    copy.start()
    copy.wait()


def late_main_kernel(
    flags, main, fresh, top, bot, gains, shifts, k1, k2, _, blocks, strips, x3, h3, row, out, sems
):
    rows, cols, chan = fresh.shape
    inner = cols - 4

    @pl.when(flags[4] == 1)
    def _():
        for p in range(rows + 4):
            row[p] = extended_row(fresh, top, bot, p - 2, 2, 4)

    @pl.when(flags[4] == 0)
    def _():
        for p in range(rows + 4):
            row[p, 0:2] = jnp.zeros((2, chan), F32)
            row[p, 2 : cols - 2] = main[inner * p : inner * (p + 1)].astype(F32)
            row[p, cols - 2 : cols] = jnp.zeros((2, chan), F32)

    for p in range(rows + 4):
        stack_row(x3, p, row[p])

    copies = []

    def emit(i, values):
        for r, value in enumerate(values):
            out[i + r] = value.astype(BF16)
            strips[0, i + r] = value[0:8]
            strips[1, i + r] = value[cols - 8 : cols]
        size = len(values)
        copy = pltpu.make_async_copy(
            out.at[pl.ds(i, size)], blocks.at[pl.ds(rows + i, size)], sems.at[len(copies)]
        )
        copy.start()
        copies.append(copy)

    weights = gains, shifts, k1, k2
    convolutions(flags, rows, cols, 0, 0, rows, x3, h3, weights, emit)
    for copy in copies:
        copy.wait()


def late_side_kernel(
    flags, main, sides, strips, fresh, top, bot, left, right, gains, shifts, k1, k2, _, blocks, x3, h3, row,
    full, osc, sems
):
    rows, cols, _ = fresh.shape
    inner = cols - 4
    wide = 4 * (rows + 8)

    @pl.when(flags[4] == 1)
    def _():
        for p in range(rows + 4):
            own = extended_row(fresh, top, bot, p - 2, 2, 4)
            spot = wide + 2 * p
            row[p, 0:2] = left[spot : spot + 2].astype(F32)
            row[p, 2:8] = own[0:6]
            row[p, 8:14] = own[cols - 6 : cols]
            row[p, 14:16] = right[spot : spot + 2].astype(F32)

    @pl.when(flags[4] == 0)
    def _():
        for p in range(rows + 4):
            edge = sides[8 * p : 8 * p + 8].astype(F32)
            row[p, 0:4] = edge[0:4]
            row[p, 4:8] = main[inner * p : inner * p + 4].astype(F32)
            row[p, 8:12] = main[inner * (p + 1) - 4 : inner * (p + 1)].astype(F32)
            row[p, 12:16] = edge[4:8]

    for p in range(rows + 4):
        stack_row(x3, p, row[p])
    copies = []

    def emit(i, values):
        for r, value in enumerate(values):
            n = i + r
            full[0, n] = strips[0, n]
            full[0, n, 0:4] = value[2:6]
            full[1, n] = strips[1, n]
            full[1, n, 4:8] = value[10:14]
            osc[0, n] = full[0, n].astype(BF16)
            osc[1, n] = full[1, n].astype(BF16)
        size = len(values)
        for side, at in enumerate((0, cols - 8)):
            copy = pltpu.make_async_copy(
                osc.at[side, pl.ds(i, size)],
                blocks.at[pl.ds(rows + i, size), pl.ds(at, 8)],
                sems.at[len(copies)],
            )
            copy.start()
            copies.append(copy)

    weights = gains, shifts, k1, k2
    convolutions(flags, rows, SIDE, 2, 0, rows, x3, h3, weights, emit)
    for copy in copies:
        copy.wait()


SMEM = pl.BlockSpec(memory_space=pltpu.SMEM)
VM = pl.BlockSpec(memory_space=pltpu.VMEM)
ANY = pl.BlockSpec(memory_space=pl.ANY)
HBM = pl.BlockSpec(memory_space=pltpu.HBM)
PARAMS = dict(vmem_limit_bytes=VMEM_LIMIT)


def cost(count, pitch, chan):
    return pl.CostEstimate(
        flops=4 * 9 * count * pitch * chan * chan, bytes_accessed=3 * 1024 * 1024, transcendentals=0
    )


def tick_call(body, operands, out_shape, count, pitch, scratch, block=False, strips=()):
    chan = out_shape[-1]
    stacks = [
        pltpu.VMEM(((count + 4) * pitch, 3 * chan), BF16),
        pltpu.VMEM(((count + 2) * pitch, 3 * chan), BF16),
    ]
    spaces = [SMEM] + [VM] * (len(operands) - 1)
    if block:
        spaces[-1] = HBM
    shapes = [jax.ShapeDtypeStruct(out_shape, BF16), *(jax.ShapeDtypeStruct(s, F32) for s in strips)]
    targets = [HBM if block else VM] + [VM] * len(strips)
    return pl.pallas_call(
        body,
        out_shape=shapes if strips else shapes[0],
        in_specs=spaces,
        out_specs=targets if strips else targets[0],
        scratch_shapes=stacks + scratch,
        input_output_aliases={len(operands) - 1: 0} if block else {},
        compiler_params=pltpu.CompilerParams(**PARAMS),
        cost_estimate=cost(count, pitch, chan),
    )(*operands)


def edge_call(x, fresh):
    shape = jax.ShapeDtypeStruct((6,) + x.shape[1:], BF16)
    return pl.pallas_call(
        edge_kernel,
        out_shape=[shape, shape],
        in_specs=[HBM, HBM],
        out_specs=[VM, VM],
        scratch_shapes=[pltpu.SemaphoreType.DMA((4,))],
        compiler_params=pltpu.CompilerParams(**PARAMS),
        name="edge",
    )(x, fresh)


def load_call(fresh, values):
    rows, _, chan = fresh.shape
    shapes = [(rows, 8, chan)] * 2 + [v.shape for v in values]
    kinds = [BF16] * 2 + [v.dtype for v in values]
    return pl.pallas_call(
        load_kernel,
        out_shape=[jax.ShapeDtypeStruct(shape, kind) for shape, kind in zip(shapes, kinds)],
        in_specs=[HBM] * (len(values) + 1),
        out_specs=[VM] * len(shapes),
        scratch_shapes=[pltpu.SemaphoreType.DMA((len(shapes),))],
        compiler_params=pltpu.CompilerParams(**PARAMS),
        cost_estimate=pl.CostEstimate(flops=1 << 30, bytes_accessed=4 << 20, transcendentals=0),
        name="load",
    )(fresh, *values)


def pack_call(x, sides, top, bot):
    rows, _, chan = x.shape
    total = 4 * (rows + 8) + 2 * (rows + 4)
    return pl.pallas_call(
        pack_kernel,
        out_shape=[jax.ShapeDtypeStruct((total, chan), BF16)] * 2,
        in_specs=[VM] * 5,
        out_specs=[VM, VM],
        scratch_shapes=[pltpu.VMEM((total, chan), F32)],
        compiler_params=pltpu.CompilerParams(**PARAMS),
        name="pack",
    )(x, *sides, top, bot)


def keep_call(main, sides, shape):
    rows, cols, chan = shape
    return pl.pallas_call(
        functools.partial(keep_kernel, rows=rows, cols=cols),
        out_shape=jax.ShapeDtypeStruct((2 * rows, cols, chan), BF16),
        in_specs=[VM, VM],
        out_specs=HBM,
        scratch_shapes=[
            pltpu.VMEM(shape, BF16),
            pltpu.VMEM(shape, F32),
            pltpu.SemaphoreType.DMA,
        ],
        compiler_params=pltpu.CompilerParams(**PARAMS),
        name="keep",
    )(main, sides)


def moves(axis, by):
    size = lax.axis_size(axis)
    return [(i, i + by) for i in range(size) if 0 <= i + by < size]


def tied(value, after):
    return lax.optimization_barrier((value, after))[0]


def in_hbm(value):
    return pltpu.with_memory_space_constraint(value, pltpu.HBM)


def per_device(state, fresh, conv_first, conv_second, gains, shifts):
    x = state[0]
    rows, cols, chan = x.shape
    flat = (9 * chan, chan)
    values = (fresh, x, gains[0], shifts[0], conv_first[0].reshape(flat), conv_second[0].reshape(flat))
    values = [in_hbm(v) for v in values]
    row, col = lax.axis_index("row"), lax.axis_index("col")
    flags = jnp.stack(
        [
            row == 0,
            row == lax.axis_size("row") - 1,
            col == 0,
            col == lax.axis_size("col") - 1,
            lax.axis_index("section") == 0,
        ]
    ).astype(jnp.int32)
    down, up = edge_call(values[1], values[0])
    bot = lax.ppermute(up, "row", moves("row", -1))
    top = lax.ppermute(down, "row", moves("row", 1))
    *sides, x, gain, shift, k1, k2 = load_call(values[0], values[1:])
    params = gain, shift, k1, k2
    tall = rows + 4

    def rows_of(*shape):
        return pltpu.VMEM((*shape, chan), F32)

    inner = tall * (cols - 4)
    operands = (flags, x, top, bot, *params)
    main = tick_call(main_kernel, operands, (inner, chan), tall, cols, [rows_of(inner)])

    def onward(message):
        return lax.ppermute(message, "section", moves("section", 1))

    got_main = onward(main)
    to_right, to_left = pack_call(x, sides, tied(top, main), bot)
    left = lax.ppermute(to_right, "col", moves("col", 1))
    right = lax.ppermute(to_left, "col", moves("col", -1))
    operands = (flags, x, top, bot, left, right, *params)
    scratch = [rows_of(8 * tall), rows_of(rows + 8, SIDE)]
    side = tick_call(side_kernel, operands, (8 * tall, chan), tall, SIDE, scratch)
    got_side = onward(side)
    blocks = keep_call(main, side, x.shape)
    operands = (flags, got_main, fresh, top, bot, *params, blocks)
    scratch = [
        rows_of(tall, cols),
        pltpu.VMEM(x.shape, BF16),
        pltpu.SemaphoreType.DMA((rows,)),
    ]
    blocks, strips = tick_call(
        late_main_kernel, operands, blocks.shape, rows, cols, scratch, block=True, strips=((2, rows, 8, chan),)
    )
    operands = (flags, got_main, got_side, strips, fresh, top, bot, left, right, *params, blocks)
    scratch = [
        rows_of(tall, SIDE),
        rows_of(2, rows, 8),
        pltpu.VMEM((2, rows, 8, chan), BF16),
        pltpu.SemaphoreType.DMA((rows,)),
    ]
    blocks = tick_call(late_side_kernel, operands, blocks.shape, rows, SIDE, scratch, block=True)
    return blocks.reshape(2, 1, rows, cols, chan)


def solution(mesh):
    in_specs = (
        P("section", "row", "col", None),
        P("row", "col", None),
        P("section", None, None, None, None),
        P("section", None, None, None, None),
        P("section", None, None),
        P("section", None, None),
    )
    out_specs = P(None, "section", "row", "col", None)
    return jax.shard_map(
        per_device, mesh=mesh, in_specs=in_specs, out_specs=out_specs, check_vma=False
    )
```
